256 devices in a mesh: tok: 8 (over x, core), col: 32 (over y, z).
Axes of the slice: x: 4, y: 4, z: 8, core: 2. Of those that a mesh axis runs over, the one named last changes fastest.
Arguments:
- hidden_in: bfloat16 [2048, 36864], P('tok', 'col'), may hold values from -6 to 6
- down_weight: bfloat16 [4608, 36864], P('col', 'tok'), may hold values from -0.046875 to 0.046875
- keep_mask: int32 [4608, 36864], P('col', 'tok'), may hold values 0 or 1
Outputs:
- layer_out: bfloat16 [2048, 4608], P(('tok', 'col'))
- hessian: float32 [4608, 4608], P('col', 'tok')
The draws below stay inside these ranges and needn't reach their ends.
All inputs are finite; a program needn't handle non-finite values. No bound on the sum of `keep_mask` on one device may be relied on, other than what follows from the above.
Results may differ from the reference program's by a relative error of at most 0.012.
Values may be sent and summed in bfloat16 or wider, within the bound.
A program may use at most 128 MiB of HBM per device.

```python
import jax
import jax.numpy as jnp
from jax import lax

D = 4608
FF = 36864
TOKENS = 2048


def touch_ends(array, stream_key, least, top_value):
    extent = array.shape
    index_at = [jax.random.randint(jax.random.fold_in(stream_key, axis), (), 0, extent[axis]) for axis in range(len(extent))]
    array = array.at[tuple(index_at)].set(least)
    longest = extent.index(max(extent))
    index_at[longest] = (index_at[longest] + 1) % extent[longest]
    return array.at[tuple(index_at)].set(top_value)


def block_scale(rng, shape, cuts, least, largest):
    factor_of, own = 1.0, jax.random.fold_in(rng, 6)
    for axis_at, blocks in cuts:
        heights = jnp.exp(jax.random.uniform(jax.random.fold_in(own, axis_at), (blocks,), jnp.float32, least / len(cuts), largest / len(cuts)))
        factor_of = factor_of * jnp.repeat(heights, shape[axis_at] // blocks).reshape([-1 if axis == axis_at else 1 for axis in range(len(shape))])
    return factor_of


def scatter_about(stream_key, dims, spread, limit, shards=(), held_as=jnp.bfloat16):
    result = spread * jax.random.normal(stream_key, dims, jnp.float32)
    if shards:
        result = result * block_scale(stream_key, dims, shards, -0.22, 0.18)
    return jnp.clip(result, -limit, limit).astype(held_as)


def setup_inputs(seed: int = 0) -> dict:
    arg_keys = jax.random.split(jax.random.key(seed), 4)
    return {
        "hidden_in": scatter_about(arg_keys[0], (TOKENS, FF), 1.0, 6.0, ((0, 8), (1, 32))),
        "down_weight": scatter_about(arg_keys[1], (D, FF), (FF // 2) ** -0.5, 0.046875, ((0, 32), (1, 8))),
        "keep_mask": touch_ends((jax.random.randint(arg_keys[2], (D, FF), 0, 2) < 1).astype(jnp.int32), jax.random.fold_in(arg_keys[2], 1), 0, 1),
    }


def reference(hidden_in, down_weight, keep_mask):
    pruned = down_weight * keep_mask.astype(down_weight.dtype)
    layer_out = lax.dot_general(hidden_in, pruned, (((1,), (1,)), ((), ())), preferred_element_type=jnp.float32).astype(jnp.bfloat16)
    hessian = jnp.dot(layer_out.T, layer_out, preferred_element_type=jnp.float32) * (2.0 / TOKENS)
    return layer_out, hessian
```

```python
import jax
import jax.numpy as jnp
from jax import lax
from jax.experimental import pallas as pl
from jax.experimental.pallas import tpu as pltpu
from jax.sharding import PartitionSpec as P

MESH = pl.DeviceIdType.MESH
NX, NY, NZ = 4, 4, 8
BF = jnp.bfloat16
F32 = jnp.float32


def dot_nt(left, right):
    return lax.dot_general(
        left, right, (((1,), (1,)), ((), ())), preferred_element_type=F32
    )


def kernel(
    scaling,
    hid, wgt, msk,
    hout, lout,
    wbuf, mbuf, bsend, bfull, abuf, csend, cown, crecv, zsend, zrecv,
    lacc, lt, rows, cols, ls, lz, lrecv, hsend, hrecv,
    in_sem, a1s, a1r, a2s, a2r, bs, br, rel_s, cs, cr, zs, zr,
    ts, tr, rs, rr, ccs, ccr, l1s, l1r, l2s, l2r, hs, hr,
):
    t = lax.axis_index("tok")
    c = lax.axis_index("col")
    x, k = t // 2, lax.rem(t, 2)
    y, z = c // NZ, lax.rem(c, NZ)
    home = z // 4
    ntok = hid.shape[0]
    half = ntok // 2
    kb = hid.shape[1]
    nb = wgt.shape[0]

    def dev(xx, kk, yy, zz):
        return (xx * 2 + kk, yy * NZ + zz)

    def remote(src, dst, ssem, rsem, to):
        return pltpu.make_async_remote_copy(
            src_ref=src, dst_ref=dst, send_sem=ssem, recv_sem=rsem,
            device_id=to, device_id_type=MESH,
        )

    me = dev(x, k, y, z)

    def arrived(dst, rsem):
        remote(dst, dst, rsem, rsem, me).wait_recv()

    def sent(src, ssem):
        remote(src, src, ssem, ssem, me).wait_send()

    aslot = jnp.where(y == x, 4 + x, y)
    for q in range(2):
        pltpu.make_async_copy(
            hid.at[pl.ds(q * half, half)], abuf.at[aslot, pl.ds(q * half, half)], in_sem.at[q]
        ).start()
    for j in range(4):
        pltpu.make_async_copy(wgt.at[:, pl.ds(j * kb, kb)], wbuf.at[j], in_sem.at[2 + j]).start()
        pltpu.make_async_copy(msk.at[:, pl.ds(j * kb, kb)], mbuf.at[j], in_sem.at[6 + j]).start()

    bar = pltpu.get_barrier_semaphore()
    for f in range(1, 8):
        pl.semaphore_signal(bar, inc=1, device_id=(lax.rem(t + f, 8), c), device_id_type=MESH)
    for d in range(1, NY):
        pl.semaphore_signal(bar, inc=1, device_id=dev(x, k, lax.rem(y + d, NY), z), device_id_type=MESH)
    for d in range(1, NZ):
        for kk in range(2):
            pl.semaphore_signal(bar, inc=1, device_id=dev(x, kk, y, lax.rem(z + d, NZ)), device_id_type=MESH)

    @pl.when(x != y)
    def _():
        pl.semaphore_signal(bar, inc=1, device_id=dev(y, k, x, z), device_id_type=MESH)

    pl.semaphore_wait(bar, jnp.where(x == y, 24, 25))

    def a1(q, d):
        return remote(
            abuf.at[aslot, pl.ds(q * half, half)], abuf.at[aslot, pl.ds(q * half, half)],
            a1s.at[q, d], a1r.at[q, y], dev(x, k, lax.rem(y + d, NY), z),
        )

    def a2(q, ys):
        return remote(
            abuf.at[ys, pl.ds(q * half, half)], abuf.at[4 + x, pl.ds(q * half, half)],
            a2s.at[q, ys], a2r.at[q, x], dev(ys, k, y, z),
        )

    for q in range(2):
        pltpu.make_async_copy(
            hid.at[pl.ds(q * half, half)], abuf.at[aslot, pl.ds(q * half, half)], in_sem.at[q]
        ).wait()
        for d in (2, 1, 3):
            a1(q, d).start()

        @pl.when(y != x)
        def _():
            a2(q, y).start()

    for j in range(4):
        pltpu.make_async_copy(wgt.at[:, pl.ds(j * kb, kb)], wbuf.at[j], in_sem.at[2 + j]).wait()
        pltpu.make_async_copy(msk.at[:, pl.ds(j * kb, kb)], mbuf.at[j], in_sem.at[6 + j]).wait()
        zt = 4 * k + j
        val = wbuf[j] * mbuf[j].astype(BF)
        bsend[j] = val

        @pl.when(zt == z)
        def _():
            bfull[z] = bsend[j]

        @pl.when(zt != z)
        def _():
            remote(bsend.at[j], bfull.at[z], bs.at[j], br.at[z], dev(x, k, y, zt)).start()

    for q in range(2):
        for d in (1, 3, 2):
            ys = lax.rem(y + d, NY)
            slot = jnp.where(ys == x, 4 + x, ys)
            arrived(abuf.at[slot, pl.ds(q * half, half)], a1r.at[q, ys])

            @pl.when(ys != x)
            def _():
                a2(q, ys).start()

    def zpart(i):
        return lax.rem(z + jnp.where(lax.rem(i, 2) == 1, (i + 1) // 2, NZ - i // 2), NZ)

    def relay(i, _):
        zq = zpart(i)

        @pl.when(jnp.logical_or(k != home, i > 0))
        def _():
            arrived(bfull.at[zq], br.at[zq])

        @pl.when(k == home)
        def _():
            remote(bfull.at[zq], bfull.at[zq], rel_s.at[zq], br.at[zq], dev(x, 1 - k, y, z)).start()

        return 0

    lax.fori_loop(0, NZ, relay, 0)

    for q in range(2):
        for e in range(1, NX):
            xs = lax.rem(x + e, NX)
            arrived(abuf.at[4 + xs, pl.ds(q * half, half)], a2r.at[q, xs])

    def product(i, _):
        zq = zpart(i)
        for e in (2, 1, 3, 0):
            x2 = lax.rem(x + e, NX)
            part = dot_nt(bfull[zq], abuf[4 + x2])
            if e == 0:
                cown[zq] = part
            else:
                csend[e - 1, zq] = part.astype(BF)
                remote(
                    csend.at[e - 1, zq], crecv.at[x, zq], cs.at[e - 1, zq], cr.at[x, zq],
                    dev(x2, k, y, z),
                ).start()
        return 0

    lax.fori_loop(0, NZ, product, 0)

    def reduce_x(i):
        zq = zpart(i)
        acc = cown[zq]
        for e in range(1, NX):
            xs = lax.rem(x + e, NX)
            arrived(crecv.at[xs, zq], cr.at[xs, zq])
            acc = acc + crecv[xs, zq].astype(F32)
        return zq, acc

    def reduce_send(i, _):
        zq, acc = reduce_x(i)
        zsend[zq] = acc.astype(BF)
        remote(zsend.at[zq], zrecv.at[z], zs.at[zq], zr.at[z], dev(x, k, y, zq)).start()
        return 0

    lax.fori_loop(1, NZ, reduce_send, 0)
    _, acc = reduce_x(0)
    lacc[...] = acc

    def reduce_z(d, _):
        zq = lax.rem(z + d, NZ)
        arrived(zrecv.at[zq], zr.at[zq])
        lacc[...] += zrecv[zq].astype(F32)
        return 0

    lax.fori_loop(1, NZ, reduce_z, 0)
    lt[...] = lacc[...].astype(BF)

    @pl.when(x != y)
    def _():
        remote(lt, rows.at[y, k], ts, tr, dev(y, k, x, z)).start()

    @pl.when(x == y)
    def _():
        rows[x, k] = lt[...]

    ident = (
        lax.broadcasted_iota(jnp.int32, (ntok, ntok), 0)
        == lax.broadcasted_iota(jnp.int32, (ntok, ntok), 1)
    ).astype(F32).astype(BF)
    ls[...] = dot_nt(ident, lt[...]).reshape(NY, NZ, 8, nb).astype(BF)
    for d in range(1, NZ):
        z2 = lax.rem(z + d, NZ)
        remote(ls.at[:, z2], lz.at[:, z], l1s.at[d], l1r.at[z], dev(x, k, y, z2)).start()
    lz[:, z] = ls[:, z]

    @pl.when(x != y)
    def _():
        arrived(rows.at[x, k], tr)

    def tok_send(f):
        t2 = lax.rem(t + f, 8)
        return remote(rows.at[x, k], rows.at[x, k], rs.at[f], rr.at[t], (t2, c))

    zrow = lax.rem(z, 4) * nb

    def col_send(d):
        return remote(
            rows.at[x, k], cols.at[k, pl.ds(zrow, nb)], ccs.at[d], ccr.at[k, lax.rem(z, 4)],
            dev(x, home, y, lax.rem(z + d, NZ)),
        )

    for d in (4, 3, 5, 2, 6, 1, 7):
        col_send(d).start()

    @pl.when(k != home)
    def _():
        col_send(0).start()

    @pl.when(k == home)
    def _():
        cols[k, pl.ds(zrow, nb)] = rows[x, k]

    for f in (4, 5, 2, 3, 6, 7, 1):
        tok_send(f).start()

    for d in range(1, NZ):
        zq = lax.rem(z + d, NZ)
        arrived(lz.at[:, zq], l1r.at[zq])
    for d in range(1, NY):
        y2 = lax.rem(y + d, NY)
        remote(lz.at[y2], lrecv.at[y], l2s.at[d], l2r.at[y], dev(x, k, y2, z)).start()
    lrecv[y] = lz[y]

    for f in range(1, 8):
        t2 = lax.rem(t + f, 8)
        arrived(rows.at[t2 // 2, lax.rem(t2, 2)], rr.at[t2])
    for kk in range(2):
        for j in range(4):
            @pl.when(jnp.logical_or(4 * k + j != z, k != kk))
            def _():
                arrived(cols.at[kk, pl.ds(j * nb, nb)], ccr.at[kk, j])

    for e in (2, 1, 3, 0):
        y2 = lax.rem(y + e, NY)
        part = dot_nt(rows[y2, 0], cols[0]) + dot_nt(rows[y2, 1], cols[1])
        part = part * scaling
        if e:
            hsend[e - 1] = part.astype(BF)
            remote(hsend.at[e - 1], hrecv.at[y], hs.at[e], hr.at[y], dev(x, k, y2, z)).start()
        else:
            hout[...] = part
    for e in (1, 3, 2):
        ys = lax.rem(y + e, NY)
        arrived(hrecv.at[ys], hr.at[ys])
        hout[...] += hrecv[ys].astype(F32)

    for d in range(1, NY):
        ys = lax.rem(y + d, NY)
        arrived(lrecv.at[ys], l2r.at[ys])
    lout[...] = lrecv[...]

    for q in range(2):
        for d in range(1, NY):
            sent(abuf.at[aslot, pl.ds(q * half, half)], a1s.at[q, d])
        for ys in range(NY):

            @pl.when(ys != x)
            def _():
                sent(abuf.at[ys, pl.ds(q * half, half)], a2s.at[q, ys])

    for j in range(4):

        @pl.when(4 * k + j != z)
        def _():
            sent(bsend.at[j], bs.at[j])

    @pl.when(k == home)
    def _():
        for zq in range(NZ):
            sent(bfull.at[zq], rel_s.at[zq])

    def drain(i, _):
        for e in range(1, NX):
            sent(csend.at[e - 1, i], cs.at[e - 1, i])

        @pl.when(i != z)
        def _():
            sent(zsend.at[i], zs.at[i])

        return 0

    lax.fori_loop(0, NZ, drain, 0)

    @pl.when(x != y)
    def _():
        sent(lt, ts)

    for d in range(1, NZ):
        sent(ls.at[:, 0], l1s.at[d])
        sent(rows.at[x, k], ccs.at[d])
        sent(rows.at[x, k], rs.at[d])
    for d in range(1, NY):
        sent(lz.at[0], l2s.at[d])
        sent(hsend.at[d - 1], hs.at[d])

    @pl.when(k != home)
    def _():
        sent(rows.at[x, k], ccs.at[0])


def body(hidden_in, down_weight, keep_mask):
    ntok, kb = hidden_in.shape
    nb = down_weight.shape[0]
    scaling = 2.0 / (ntok * lax.axis_size("tok"))
    dma = pltpu.SemaphoreType.DMA
    hessian, rows = pl.pallas_call(
        lambda *refs: kernel(scaling, *refs),
        out_shape=(
            jax.ShapeDtypeStruct((nb, 4 * nb), F32),
            jax.ShapeDtypeStruct((NY, NZ, 8, nb), BF),
        ),
        in_specs=[pl.BlockSpec(memory_space=pl.ANY)] * 3,
        out_specs=(pl.BlockSpec(memory_space=pltpu.VMEM),) * 2,
        scratch_shapes=[
            pltpu.VMEM((4, nb, kb), BF),
            pltpu.VMEM((4, nb, kb), jnp.int32),
            pltpu.VMEM((4, nb, kb), BF),
            pltpu.VMEM((NZ, nb, kb), BF),
            pltpu.VMEM((8, ntok, kb), BF),
            pltpu.VMEM((3, NZ, nb, ntok), BF),
            pltpu.VMEM((NZ, nb, ntok), F32),
            pltpu.VMEM((NX, NZ, nb, ntok), BF),
            pltpu.VMEM((NZ, nb, ntok), BF),
            pltpu.VMEM((NZ, nb, ntok), BF),
            pltpu.VMEM((nb, ntok), F32),
            pltpu.VMEM((nb, ntok), BF),
            pltpu.VMEM((NX, 2, nb, ntok), BF),
            pltpu.VMEM((2, 4 * nb, ntok), BF),
            pltpu.VMEM((NY, NZ, 8, nb), BF),
            pltpu.VMEM((NY, NZ, 8, nb), BF),
            pltpu.VMEM((NY, NZ, 8, nb), BF),
            pltpu.VMEM((3, nb, 4 * nb), BF),
            pltpu.VMEM((NY, nb, 4 * nb), BF),
            dma((10,)),
            dma((2, 4)), dma((2, 4)), dma((2, 4)), dma((2, 4)),
            dma((4,)), dma((NZ,)), dma((NZ,)),
            dma((3, NZ)), dma((NX, NZ)), dma((NZ,)), dma((NZ,)),
            dma(()), dma(()),
            dma((8,)), dma((8,)), dma((8,)), dma((2, 4)),
            dma((8,)), dma((8,)), dma((4,)), dma((4,)),
            dma((4,)), dma((4,)),
        ],
        compiler_params=pltpu.CompilerParams(
            collective_id=0, has_side_effects=True, vmem_limit_bytes=60 * 2**20
        ),
    )(hidden_in, down_weight, keep_mask)
    layer_out = rows.transpose(2, 0, 1, 3).reshape(8, NY * NZ * nb)
    return layer_out, hessian


def solution(mesh):
    in_specs = (P("tok", "col"), P("col", "tok"), P("col", "tok"))
    out_specs = (P(("tok", "col"), None), P("col", "tok"))
    return jax.shard_map(body, mesh=mesh, in_specs=in_specs, out_specs=out_specs, check_vma=False)
```

```python
import jax
import jax.numpy as jnp
from jax import lax
from jax.experimental import pallas as pl
from jax.experimental.pallas import tpu as pltpu
from jax.sharding import PartitionSpec as P

MESH = pl.DeviceIdType.MESH
NX, NY, NZ = 4, 4, 8
BF = jnp.bfloat16
F32 = jnp.float32


def dot_nt(left, right):
    return lax.dot_general(
        left, right, (((1,), (1,)), ((), ())), preferred_element_type=F32
    )


def kernel(
    scaling,
    hid, wgt, msk,
    hout, lout,
    hbuf, wbuf, mbuf, bsend, bfull, abuf, csend, crecv, zsend, zrecv,
    lacc, lt, rows, cols, ls, lz, lrecv, hsend, hrecv,
    in_sem, y1s, y1r, xs_s, xs_r, y2s, y2r, y3s, bs, br, rel_s, cs, cr, zs, zr,
    ts, tr, rs, rr, ccs, ccr, l1s, l1r, l2s, l2r, hs, hr,
):
    t = lax.axis_index("tok")
    c = lax.axis_index("col")
    x, k = t // 2, lax.rem(t, 2)
    y, z = c // NZ, lax.rem(c, NZ)
    home = z // 4
    ntok = hid.shape[0]
    half = ntok // 2
    kb = hid.shape[1]
    nb = wgt.shape[0]

    def dev(xx, kk, yy, zz):
        return (xx * 2 + kk, yy * NZ + zz)

    def remote(src, dst, ssem, rsem, to):
        return pltpu.make_async_remote_copy(
            src_ref=src, dst_ref=dst, send_sem=ssem, recv_sem=rsem,
            device_id=to, device_id_type=MESH,
        )

    me = dev(x, k, y, z)

    def arrived(dst, rsem):
        remote(dst, dst, rsem, rsem, me).wait_recv()

    def sent(src, ssem):
        remote(src, src, ssem, ssem, me).wait_send()

    aslot = jnp.where(y == x, 4 + x, y)
    holder = y // 2 == k
    hown = jnp.where(holder, y - 2 * k, 0)

    def load_piece(h, own):
        rows_h = pl.ds(h * half, half)
        dst = abuf.at[aslot, rows_h] if own else hbuf.at[rows_h]
        return pltpu.make_async_copy(hid.at[rows_h], dst, in_sem.at[h])

    def load_weight(j):
        return (
            pltpu.make_async_copy(wgt.at[:, pl.ds(j * kb, kb)], wbuf.at[j], in_sem.at[2 + j]),
            pltpu.make_async_copy(msk.at[:, pl.ds(j * kb, kb)], mbuf.at[j], in_sem.at[6 + j]),
        )

    for h in range(2):

        @pl.when(y == 2 * k + h)
        def _():
            load_piece(h, True).start()

        @pl.when(y != 2 * k + h)
        def _():
            load_piece(h, False).start()

    for j in range(4):
        for copy in load_weight(j):
            copy.start()

    bar = pltpu.get_barrier_semaphore()
    for f in range(1, 8):
        pl.semaphore_signal(bar, inc=1, device_id=(lax.rem(t + f, 8), c), device_id_type=MESH)
    for d in range(1, NY):
        pl.semaphore_signal(bar, inc=1, device_id=dev(x, k, lax.rem(y + d, NY), z), device_id_type=MESH)
    for d in range(1, NZ):
        for kk in range(2):
            pl.semaphore_signal(bar, inc=1, device_id=dev(x, kk, y, lax.rem(z + d, NZ)), device_id_type=MESH)

    @pl.when(x != y)
    def _():
        pl.semaphore_signal(bar, inc=1, device_id=dev(y, k, x, z), device_id_type=MESH)

    pl.semaphore_wait(bar, jnp.where(x == y, 24, 25))

    for h in range(2):

        @pl.when(y == 2 * k + h)
        def _():
            load_piece(h, True).wait()

        @pl.when(y != 2 * k + h)
        def _():
            load_piece(h, False).wait()
            remote(
                hbuf.at[pl.ds(h * half, half)], abuf.at[aslot, pl.ds(h * half, half)],
                y1s.at[h], y1r.at[y], dev(x, k, 2 * k + h, z),
            ).start()

    def zpart(i):
        return lax.rem(z + jnp.where(lax.rem(i, 2) == 1, (i + 1) // 2, NZ - i // 2), NZ)

    def prune(i, _):
        zt = zpart(i)

        @pl.when(zt // 4 == k)
        def _():
            j = lax.rem(zt, 4)
            for copy in load_weight_at(j):
                copy.wait()
            bsend[j] = wbuf[j] * mbuf[j].astype(BF)

            @pl.when(zt == z)
            def _():
                bfull[z] = bsend[j]

            @pl.when(zt != z)
            def _():
                remote(bsend.at[j], bfull.at[z], bs.at[j], br.at[z], dev(x, k, y, zt)).start()

        return 0

    def load_weight_at(j):
        return (
            pltpu.make_async_copy(wgt.at[:, pl.ds(0, kb)], wbuf.at[j], in_sem.at[2 + j]),
            pltpu.make_async_copy(msk.at[:, pl.ds(0, kb)], mbuf.at[j], in_sem.at[6 + j]),
        )

    lax.fori_loop(0, NZ, prune, 0)

    order = (2, 1, 3, 0)
    quarter = half // 2

    def piece(slot, h, part=None):
        if part is None:
            return abuf.at[slot, pl.ds(h * half, half)]
        return abuf.at[slot, pl.ds(h * half + part * quarter, quarter)]

    def handed(e, h, part, ssem, up):
        slot = 4 + lax.rem(x + e, NX)
        return remote(
            piece(slot, h, part), piece(slot, h, part), ssem, y2r.at[h, e, part],
            dev(x, k, lax.rem(y + (1 if up else NY - 1), NY), z),
        )

    @pl.when(holder)
    def _():
        for e in (2, 1, 3):
            ys = lax.rem(x + NX - e, NX)

            @pl.when(ys != y)
            def _():
                arrived(piece(ys, hown), y1r.at[ys])

            remote(piece(ys, hown), piece(4 + x, hown), xs_s.at[e], xs_r.at[x], dev(ys, k, y, z)).start()
        for e in order:
            xe = lax.rem(x + e, NX)
            if e:
                arrived(piece(4 + xe, hown), xs_r.at[xe])
            else:

                @pl.when(x != y)
                def _():
                    arrived(piece(4 + x, hown), y1r.at[x])

            for m, (part, up) in enumerate(((0, True), (1, False), (1, True), (0, False))):
                handed(e, hown, part, y2s.at[e, m], up).start()

    def relay_tokens(e):
        for h in range(2):
            away = lax.rem(y + NY - 2 * k - h + NY, NY)

            @pl.when(away == 1)
            def _():
                arrived(piece(4 + lax.rem(x + e, NX), h, 0), y2r.at[h, e, 0])
                handed(e, h, 0, y3s.at[e, h], True).start()

            @pl.when(away == 3)
            def _():
                arrived(piece(4 + lax.rem(x + e, NX), h, 1), y2r.at[h, e, 1])
                handed(e, h, 1, y3s.at[e, h], False).start()

    def tokens_here(e):
        for h in range(2):
            away = lax.rem(y + NY - 2 * k - h + NY, NY)

            @pl.when(away >= 2)
            def _():
                arrived(piece(4 + lax.rem(x + e, NX), h, 0), y2r.at[h, e, 0])

            @pl.when(jnp.logical_or(away == 1, away == 2))
            def _():
                arrived(piece(4 + lax.rem(x + e, NX), h, 1), y2r.at[h, e, 1])

    def relay_weights(i, _):
        zq = zpart(i)

        @pl.when(jnp.logical_or(k != home, i > 0))
        def _():
            arrived(bfull.at[zq], br.at[zq])

        @pl.when(k == home)
        def _():
            remote(bfull.at[zq], bfull.at[zq], rel_s.at[zq], br.at[zq], dev(x, 1 - k, y, z)).start()

        return 0

    def products(es, lo, hi):
        def step(i, _):
            zq = zpart(i)
            for e in es:
                x2 = lax.rem(x + e, NX)
                csend[e - 1, zq] = dot_nt(bfull[zq], abuf[4 + x2]).astype(BF)
                remote(
                    csend.at[e - 1, zq], crecv.at[x, zq], cs.at[e - 1, zq], cr.at[x, zq],
                    dev(x2, k, y, z),
                ).start()
            return 0

        lax.fori_loop(lo, hi, step, 0)

    for n, e in enumerate(order):
        relay_tokens(e)
        lax.fori_loop(2 * n, 2 * n + 2, relay_weights, 0)
        if n:
            products(order[:n], 2 * n, 2 * n + 2)
        tokens_here(e)
        if e:
            products((e,), 0, 2 * n + 2)

    def reduce_x(i):
        zq = zpart(i)
        acc = dot_nt(bfull[zq], abuf[4 + x])
        for e in range(1, NX):
            xs = lax.rem(x + e, NX)
            arrived(crecv.at[xs, zq], cr.at[xs, zq])
            acc = acc + crecv[xs, zq].astype(F32)
        return zq, acc

    def reduce_send(i, _):
        zq, acc = reduce_x(i)
        zsend[zq] = acc.astype(BF)
        remote(zsend.at[zq], zrecv.at[z], zs.at[zq], zr.at[z], dev(x, k, y, zq)).start()
        return 0

    lax.fori_loop(1, NZ, reduce_send, 0)
    _, acc = reduce_x(0)
    lacc[...] = acc

    def reduce_z(d, _):
        zq = lax.rem(z + d, NZ)
        arrived(zrecv.at[zq], zr.at[zq])
        lacc[...] += zrecv[zq].astype(F32)
        return 0

    lax.fori_loop(1, NZ, reduce_z, 0)
    lt[...] = lacc[...].astype(BF)

    @pl.when(x != y)
    def _():
        remote(lt, rows.at[y, k], ts, tr, dev(y, k, x, z)).start()

    @pl.when(x == y)
    def _():
        rows[x, k] = lt[...]

    ident = (
        lax.broadcasted_iota(jnp.int32, (ntok, ntok), 0)
        == lax.broadcasted_iota(jnp.int32, (ntok, ntok), 1)
    ).astype(F32).astype(BF)
    ls[...] = dot_nt(ident, lt[...]).reshape(NY, NZ, 8, nb).astype(BF)
    for d in range(1, NZ):
        z2 = lax.rem(z + d, NZ)
        remote(ls.at[:, z2], lz.at[:, z], l1s.at[d], l1r.at[z], dev(x, k, y, z2)).start()
    lz[:, z] = ls[:, z]

    @pl.when(x != y)
    def _():
        arrived(rows.at[x, k], tr)

    def tok_send(f):
        t2 = lax.rem(t + f, 8)
        return remote(rows.at[x, k], rows.at[x, k], rs.at[f], rr.at[t], (t2, c))

    zrow = lax.rem(z, 4) * nb

    def col_send(d):
        return remote(
            rows.at[x, k], cols.at[k, pl.ds(zrow, nb)], ccs.at[d], ccr.at[k, lax.rem(z, 4)],
            dev(x, home, y, lax.rem(z + d, NZ)),
        )

    for d in (4, 3, 5, 2, 6, 1, 7):
        col_send(d).start()

    @pl.when(k != home)
    def _():
        col_send(0).start()

    @pl.when(k == home)
    def _():
        cols[k, pl.ds(zrow, nb)] = rows[x, k]

    for f in (4, 5, 2, 3, 6, 7, 1):
        tok_send(f).start()

    for d in range(1, NZ):
        zq = lax.rem(z + d, NZ)
        arrived(lz.at[:, zq], l1r.at[zq])
    for d in range(1, NY):
        y2 = lax.rem(y + d, NY)
        remote(lz.at[y2], lrecv.at[y], l2s.at[d], l2r.at[y], dev(x, k, y2, z)).start()
    lrecv[y] = lz[y]

    for f in range(1, 8):
        t2 = lax.rem(t + f, 8)
        arrived(rows.at[t2 // 2, lax.rem(t2, 2)], rr.at[t2])
    for kk in range(2):
        for j in range(4):
            @pl.when(jnp.logical_or(4 * k + j != z, k != kk))
            def _():
                arrived(cols.at[kk, pl.ds(j * nb, nb)], ccr.at[kk, j])

    for e in (2, 1, 3, 0):
        y2 = lax.rem(y + e, NY)
        part = dot_nt(rows[y2, 0], cols[0]) + dot_nt(rows[y2, 1], cols[1])
        part = part * scaling
        if e:
            hsend[e - 1] = part.astype(BF)
            remote(hsend.at[e - 1], hrecv.at[y], hs.at[e], hr.at[y], dev(x, k, y2, z)).start()
        else:
            hout[...] = part
    for e in (1, 3, 2):
        ys = lax.rem(y + e, NY)
        arrived(hrecv.at[ys], hr.at[ys])
        hout[...] += hrecv[ys].astype(F32)

    for d in range(1, NY):
        ys = lax.rem(y + d, NY)
        arrived(lrecv.at[ys], l2r.at[ys])
    lout[...] = lrecv[...]

    for h in range(2):

        @pl.when(y != 2 * k + h)
        def _():
            sent(hbuf.at[pl.ds(h * half, half)], y1s.at[h])

    @pl.when(holder)
    def _():
        for e in (1, 2, 3):
            sent(piece(4 + x, hown), xs_s.at[e])
        for e in range(4):
            for m in range(4):
                sent(piece(4 + x, hown, 0), y2s.at[e, m])

    for h in range(2):
        away = lax.rem(y + NY - 2 * k - h + NY, NY)

        @pl.when(jnp.logical_or(away == 1, away == 3))
        def _():
            for e in range(4):
                sent(piece(4 + x, h, 0), y3s.at[e, h])

    for j in range(4):

        @pl.when(4 * k + j != z)
        def _():
            sent(bsend.at[j], bs.at[j])

    @pl.when(k == home)
    def _():
        for zq in range(NZ):
            sent(bfull.at[zq], rel_s.at[zq])

    def drain(i, _):
        for e in range(1, NX):
            sent(csend.at[e - 1, i], cs.at[e - 1, i])

        @pl.when(i != z)
        def _():
            sent(zsend.at[i], zs.at[i])

        return 0

    lax.fori_loop(0, NZ, drain, 0)

    @pl.when(x != y)
    def _():
        sent(lt, ts)

    for d in range(1, NZ):
        sent(ls.at[:, 0], l1s.at[d])
        sent(rows.at[x, k], ccs.at[d])
        sent(rows.at[x, k], rs.at[d])
    for d in range(1, NY):
        sent(lz.at[0], l2s.at[d])
        sent(hsend.at[d - 1], hs.at[d])

    @pl.when(k != home)
    def _():
        sent(rows.at[x, k], ccs.at[0])


def body(hidden_in, down_weight, keep_mask):
    ntok, kb = hidden_in.shape
    nb = down_weight.shape[0]
    scaling = 2.0 / (ntok * lax.axis_size("tok"))
    dma = pltpu.SemaphoreType.DMA
    hessian, rows = pl.pallas_call(
        lambda *refs: kernel(scaling, *refs),
        out_shape=(
            jax.ShapeDtypeStruct((nb, 4 * nb), F32),
            jax.ShapeDtypeStruct((NY, NZ, 8, nb), BF),
        ),
        in_specs=[pl.BlockSpec(memory_space=pl.ANY)] * 3,
        out_specs=(pl.BlockSpec(memory_space=pltpu.VMEM),) * 2,
        scratch_shapes=[
            pltpu.VMEM((ntok, kb), BF),
            pltpu.VMEM((4, nb, kb), BF),
            pltpu.VMEM((4, nb, kb), jnp.int32),
            pltpu.VMEM((4, nb, kb), BF),
            pltpu.VMEM((NZ, nb, kb), BF),
            pltpu.VMEM((8, ntok, kb), BF),
            pltpu.VMEM((3, NZ, nb, ntok), BF),
            pltpu.VMEM((NX, NZ, nb, ntok), BF),
            pltpu.VMEM((NZ, nb, ntok), BF),
            pltpu.VMEM((NZ, nb, ntok), BF),
            pltpu.VMEM((nb, ntok), F32),
            pltpu.VMEM((nb, ntok), BF),
            pltpu.VMEM((NX, 2, nb, ntok), BF),
            pltpu.VMEM((2, 4 * nb, ntok), BF),
            pltpu.VMEM((NY, NZ, 8, nb), BF),
            pltpu.VMEM((NY, NZ, 8, nb), BF),
            pltpu.VMEM((NY, NZ, 8, nb), BF),
            pltpu.VMEM((3, nb, 4 * nb), BF),
            pltpu.VMEM((NY, nb, 4 * nb), BF),
            dma((10,)),
            dma((2,)), dma((4,)), dma((4,)), dma((4,)),
            dma((4, 4)), dma((2, 4, 2)), dma((4, 2)),
            dma((4,)), dma((NZ,)), dma((NZ,)),
            dma((3, NZ)), dma((NX, NZ)), dma((NZ,)), dma((NZ,)),
            dma(()), dma(()),
            dma((8,)), dma((8,)), dma((8,)), dma((2, 4)),
            dma((8,)), dma((8,)), dma((4,)), dma((4,)),
            dma((4,)), dma((4,)),
        ],
        compiler_params=pltpu.CompilerParams(
            collective_id=0, has_side_effects=True, vmem_limit_bytes=60 * 2**20
        ),
    )(hidden_in, down_weight, keep_mask)
    layer_out = rows.transpose(2, 0, 1, 3).reshape(8, NY * NZ * nb)
    return layer_out, hessian


def solution(mesh):
    in_specs = (P("tok", "col"), P("col", "tok"), P("col", "tok"))
    out_specs = (P(("tok", "col"), None), P("col", "tok"))
    return jax.shard_map(body, mesh=mesh, in_specs=in_specs, out_specs=out_specs, check_vma=False)
```

```python
import jax
import jax.numpy as jnp
from jax import lax
from jax.experimental import pallas as pl
from jax.experimental.pallas import tpu as pltpu
from jax.sharding import PartitionSpec as P

MESH = pl.DeviceIdType.MESH
NX, NY, NZ = 4, 4, 8
BF = jnp.bfloat16
F32 = jnp.float32


def dot_nt(left, right):
    return lax.dot_general(
        left, right, (((1,), (1,)), ((), ())), preferred_element_type=F32
    )


def kernel(
    scaling,
    hid, wgt, msk,
    hout, lout,
    hbuf, wbuf, mbuf, bsend, bfull, abuf, csend, crecv, nrecv, pbuf, zsend, zrecv,
    lacc, lt, rows, cols, ls, lz, lrecv, hsend, hrecv, hacc,
    in_sem, y1s, y1r, xs_s, xs_r, y2s, y2r, y3s, bs, br, rel_s, cs, cr, nr, zs, zr,
    ts, tr, rs, rr, ccs, ccr, l1s, l1r, l2s, l2r, hs, hr,
):
    t = lax.axis_index("tok")
    c = lax.axis_index("col")
    x, k = t // 2, lax.rem(t, 2)
    y, z = c // NZ, lax.rem(c, NZ)
    home = z // 4
    ntok = hid.shape[0]
    half = ntok // 2
    kb = hid.shape[1]
    nb = wgt.shape[0]

    def dev(xx, kk, yy, zz):
        return (xx * 2 + kk, yy * NZ + zz)

    def remote(src, dst, ssem, rsem, to):
        return pltpu.make_async_remote_copy(
            src_ref=src, dst_ref=dst, send_sem=ssem, recv_sem=rsem,
            device_id=to, device_id_type=MESH,
        )

    me = dev(x, k, y, z)

    def arrived(dst, rsem):
        remote(dst, dst, rsem, rsem, me).wait_recv()

    def sent(src, ssem):
        remote(src, src, ssem, ssem, me).wait_send()

    bar = pltpu.get_barrier_semaphore()
    for f in range(1, 8):
        pl.semaphore_signal(bar, inc=1, device_id=(lax.rem(t + f, 8), c), device_id_type=MESH)
    for d in range(1, NY):
        pl.semaphore_signal(bar, inc=1, device_id=dev(x, k, lax.rem(y + d, NY), z), device_id_type=MESH)
    for d in range(1, NZ):
        for kk in range(2):
            pl.semaphore_signal(bar, inc=1, device_id=dev(x, kk, y, lax.rem(z + d, NZ)), device_id_type=MESH)

    @pl.when(x != y)
    def _():
        pl.semaphore_signal(bar, inc=1, device_id=dev(y, k, x, z), device_id_type=MESH)

    aslot = jnp.where(y == x, 4 + x, y)
    holder = y // 2 == k
    hown = jnp.where(holder, y - 2 * k, 0)

    def load_piece(h, own):
        rows_h = pl.ds(h * half, half)
        dst = abuf.at[aslot, rows_h] if own else hbuf.at[rows_h]
        return pltpu.make_async_copy(hid.at[rows_h], dst, in_sem.at[h])

    def load_weight(j):
        return (
            pltpu.make_async_copy(wgt.at[:, pl.ds(j * kb, kb)], wbuf.at[j], in_sem.at[2 + j]),
            pltpu.make_async_copy(msk.at[:, pl.ds(j * kb, kb)], mbuf.at[j], in_sem.at[6 + j]),
        )

    for h in range(2):

        @pl.when(y == 2 * k + h)
        def _():
            load_piece(h, True).start()

        @pl.when(y != 2 * k + h)
        def _():
            load_piece(h, False).start()

    for j in range(4):
        for copy in load_weight(j):
            copy.start()

    def prune(j, _):
        for copy in load_weight_at(j):
            copy.wait()
        bsend[j] = wbuf[j] * mbuf[j].astype(BF)
        return 0

    def load_weight_at(j):
        return (
            pltpu.make_async_copy(wgt.at[:, pl.ds(0, kb)], wbuf.at[j], in_sem.at[2 + j]),
            pltpu.make_async_copy(msk.at[:, pl.ds(0, kb)], mbuf.at[j], in_sem.at[6 + j]),
        )

    lax.fori_loop(0, 4, prune, 0)

    pl.semaphore_wait(bar, jnp.where(x == y, 24, 25))

    quarter = half // 2

    for h in range(2):

        @pl.when(y == 2 * k + h)
        def _():
            load_piece(h, True).wait()

        @pl.when(y != 2 * k + h)
        def _():
            load_piece(h, False).wait()
    for part in range(2):
        for h in range(2):

            @pl.when(y != 2 * k + h)
            def _():
                rows_p = pl.ds(h * half + part * quarter, quarter)
                remote(
                    hbuf.at[rows_p], abuf.at[aslot, rows_p],
                    y1s.at[h, part], y1r.at[y, part], dev(x, k, 2 * k + h, z),
                ).start()

    def zpart(i):
        i = jnp.int32(i)
        return lax.rem(z + jnp.where(lax.rem(i, 2) == 1, (i + 1) // 2, NZ - i // 2), NZ)

    def place(d):
        return jnp.where(d == 0, 0, jnp.where(d <= 4, 2 * d - 1, 2 * (NZ - d)))

    def hand_out(i, _):
        zt = zpart(i)

        @pl.when(zt // 4 == k)
        def _():
            j = lax.rem(zt, 4)

            @pl.when(zt == z)
            def _():
                bfull[0] = bsend[j]

            @pl.when(zt != z)
            def _():
                slot = place(lax.rem(z + NZ - zt, NZ))
                remote(bsend.at[j], bfull.at[slot], bs.at[j], br.at[slot], dev(x, k, y, zt)).start()

        return 0

    lax.fori_loop(0, NZ, hand_out, 0)

    order = (2, 1, 3, 0)

    def piece(slot, h, part=None):
        if part is None:
            return abuf.at[slot, pl.ds(h * half, half)]
        return abuf.at[slot, pl.ds(h * half + part * quarter, quarter)]

    def handed(e, h, part, ssem, up):
        slot = 4 + lax.rem(x + e, NX)
        return remote(
            piece(slot, h, part), piece(slot, h, part), ssem, y2r.at[h, e, part],
            dev(x, k, lax.rem(y + (1 if up else NY - 1), NY), z),
        )

    @pl.when(holder)
    def _():
        for part in range(2):
            for e in (2, 1, 3):
                ys = lax.rem(x + NX - e, NX)

                @pl.when(ys != y)
                def _():
                    arrived(piece(ys, hown, part), y1r.at[ys, part])

                remote(
                    piece(ys, hown, part), piece(4 + x, hown, part),
                    xs_s.at[e, part], xs_r.at[x, part], dev(ys, k, y, z),
                ).start()
        for e in order:
            xe = lax.rem(x + e, NX)
            for part in range(2):
                if e:
                    arrived(piece(4 + xe, hown, part), xs_r.at[xe, part])
                else:

                    @pl.when(x != y)
                    def _():
                        arrived(piece(4 + x, hown, part), y1r.at[x, part])

                for up in (part == 0, part == 1):
                    handed(e, hown, part, y2s.at[e, part, int(up)], up).start()

    def relay_tokens(e):
        for h in range(2):
            away = lax.rem(y + NY - 2 * k - h + NY, NY)

            @pl.when(away == 1)
            def _():
                arrived(piece(4 + lax.rem(x + e, NX), h, 0), y2r.at[h, e, 0])
                handed(e, h, 0, y3s.at[e, h], True).start()

            @pl.when(away == 3)
            def _():
                arrived(piece(4 + lax.rem(x + e, NX), h, 1), y2r.at[h, e, 1])
                handed(e, h, 1, y3s.at[e, h], False).start()

    def tokens_here(e):
        for h in range(2):
            away = lax.rem(y + NY - 2 * k - h + NY, NY)

            @pl.when(away >= 2)
            def _():
                arrived(piece(4 + lax.rem(x + e, NX), h, 0), y2r.at[h, e, 0])

            @pl.when(jnp.logical_or(away == 1, away == 2))
            def _():
                arrived(piece(4 + lax.rem(x + e, NX), h, 1), y2r.at[h, e, 1])

    def relay_weights(i, _):
        @pl.when(jnp.logical_or(k != home, i > 0))
        def _():
            arrived(bfull.at[i], br.at[i])

        @pl.when(k == home)
        def _():
            remote(bfull.at[i], bfull.at[i], rel_s.at[i], br.at[i], dev(x, 1 - k, y, z)).start()

        return 0

    def product(e, lo, hi):
        left = bfull[lo:hi].reshape((hi - lo) * nb, kb)
        return dot_nt(left, abuf[4 + lax.rem(x + e, NX)]).reshape(hi - lo, nb, ntok)

    via_up = (0, 2, 4, 6, 7)

    def products(e, lo, hi, order=None):
        pbuf[lo:hi] = product(e, lo, hi)
        for i in order or range(lo, hi):
            src, ssem = csend.at[e - 1, i], cs.at[e - 1, i]
            if e == 2:
                csend[1, i] = pbuf[i].astype(BF)
                to = lax.rem(x + (1 if i in via_up else NX - 1), NX)
                remote(src, nrecv.at[i], ssem, nr.at[i], dev(to, k, y, z)).start()
                continue
            if (i in via_up) == (e == 1):
                arrived(nrecv.at[i], nr.at[i])
                csend[e - 1, i] = (pbuf[i] + nrecv[i].astype(F32)).astype(BF)
            else:
                csend[e - 1, i] = pbuf[i].astype(BF)
            remote(
                src, crecv.at[e // 2, i], ssem, cr.at[e // 2, i], dev(lax.rem(x + e, NX), k, y, z)
            ).start()

    def weights(lo, hi):
        lax.fori_loop(lo, hi, relay_weights, 0)

    relay_tokens(2)
    weights(0, 3)
    relay_tokens(1)
    tokens_here(2)
    products(2, 0, 3)
    weights(3, 5)
    products(2, 3, 5)
    relay_tokens(3)
    weights(5, 7)
    products(2, 5, 7)
    tokens_here(1)
    products(1, 0, 7, order=(1, 2, 3, 4, 5, 6, 0))
    relay_tokens(0)
    tokens_here(3)
    products(3, 0, 7, order=(1, 2, 3, 4, 5, 6, 0))
    tokens_here(0)
    pbuf[0:7] = product(0, 0, 7)

    def reduce_x(i):
        for side in range(2):
            arrived(crecv.at[side, i], cr.at[side, i])
        return pbuf[i] + crecv[0, i].astype(F32) + crecv[1, i].astype(F32)

    def reduce_send(i):
        zq = zpart(i)
        acc = reduce_x(i).astype(BF)
        for h in range(2):
            zsend[h, zq] = acc[:, h * half : (h + 1) * half]
            remote(
                zsend.at[h, zq], zrecv.at[h, z], zs.at[h, zq], zr.at[h, z], dev(x, k, y, zq)
            ).start()

    reduce_send(1)
    weights(7, 8)
    products(2, 7, 8)
    products(3, 7, 8)
    reduce_send(2)
    reduce_send(3)
    reduce_send(4)
    products(1, 7, 8)
    pbuf[7] = product(0, 7, 8)[0]
    reduce_send(5)
    reduce_send(6)
    reduce_send(7)
    acc = reduce_x(0)
    for h in range(2):
        lacc[h] = acc[:, h * half : (h + 1) * half]

    def reduce_z(h):
        lanes = pl.ds(h * half, half)

        def step(d, _):
            zq = lax.rem(z + d, NZ)
            arrived(zrecv.at[h, zq], zr.at[h, zq])
            lacc[h] += zrecv[h, zq].astype(F32)
            return 0

        lax.fori_loop(1, NZ, step, 0)
        lt[:, lanes] = lacc[h].astype(BF)

        @pl.when(x != y)
        def _():
            remote(lt.at[:, lanes], rows.at[y, k, :, lanes], ts.at[h], tr.at[h], dev(y, k, x, z)).start()

        @pl.when(x == y)
        def _():
            rows[x, k, :, lanes] = lt[:, lanes]

    zrow = lax.rem(z, 4) * nb

    def tok_send(f, h):
        t2 = lax.rem(t + f, 8)
        mine = rows.at[x, k, :, pl.ds(h * half, half)]
        return remote(mine, mine, rs.at[h, f], rr.at[h, t], (t2, c))

    def col_send(d, h):
        lanes = pl.ds(h * half, half)
        return remote(
            rows.at[x, k, :, lanes], cols.at[k, pl.ds(zrow, nb), lanes],
            ccs.at[h, d], ccr.at[h, k, lax.rem(z, 4)],
            dev(x, home, y, lax.rem(z + d, NZ)),
        )

    def spread(h):
        lanes = pl.ds(h * half, half)

        @pl.when(x != y)
        def _():
            arrived(rows.at[x, k, :, lanes], tr.at[h])

        for d in (4, 3, 5, 2, 6, 1, 7):
            col_send(d, h).start()

        @pl.when(k != home)
        def _():
            col_send(0, h).start()

        @pl.when(k == home)
        def _():
            cols[k, pl.ds(zrow, nb), lanes] = rows[x, k, :, lanes]

        for f in (4, 5, 2, 3, 6, 7, 1):
            tok_send(f, h).start()

    reduce_z(0)
    reduce_z(1)
    spread(0)

    ident = (
        lax.broadcasted_iota(jnp.int32, (ntok, ntok), 0)
        == lax.broadcasted_iota(jnp.int32, (ntok, ntok), 1)
    ).astype(F32).astype(BF)
    ls[...] = dot_nt(ident, lt[...]).reshape(NY, NZ, 8, nb).astype(BF)
    for d in range(1, NZ):
        z2 = lax.rem(z + d, NZ)
        remote(ls.at[:, z2], lz.at[:, z], l1s.at[d], l1r.at[z], dev(x, k, y, z2)).start()
    lz[:, z] = ls[:, z]

    spread(1)

    for d in range(1, NZ):
        zq = lax.rem(z + d, NZ)
        arrived(lz.at[:, zq], l1r.at[zq])
    for d in range(1, NY):
        y2 = lax.rem(y + d, NY)
        remote(lz.at[y2], lrecv.at[y], l2s.at[d], l2r.at[y], dev(x, k, y2, z)).start()
    lrecv[y] = lz[y]

    for f in range(1, 8):
        t2 = lax.rem(t + f, 8)
        for h in range(2):
            arrived(rows.at[t2 // 2, lax.rem(t2, 2), :, pl.ds(h * half, half)], rr.at[h, t2])
    for kk in range(2):
        for j in range(4):
            @pl.when(jnp.logical_or(4 * k + j != z, k != kk))
            def _():
                for h in range(2):
                    arrived(cols.at[kk, pl.ds(j * nb, nb), pl.ds(h * half, half)], ccr.at[h, kk, j])

    part = sum(dot_nt(rows[:, kk].reshape(NY * nb, ntok), cols[kk]) for kk in range(2))
    hacc[...] = (part * scaling).reshape(NY, nb, NY * nb)
    for e in (2, 1, 3):
        y2 = lax.rem(y + e, NY)
        hsend[e - 1] = hacc[y2].astype(BF)
        remote(hsend.at[e - 1], hrecv.at[y], hs.at[e], hr.at[y], dev(x, k, y2, z)).start()
    hout[...] = hacc[y]
    for e in (1, 3, 2):
        ys = lax.rem(y + e, NY)
        arrived(hrecv.at[ys], hr.at[ys])
        hout[...] += hrecv[ys].astype(F32)

    for d in range(1, NY):
        ys = lax.rem(y + d, NY)
        arrived(lrecv.at[ys], l2r.at[ys])
    lout[...] = lrecv[...]

    for h in range(2):

        @pl.when(y != 2 * k + h)
        def _():
            for part in range(2):
                sent(hbuf.at[pl.ds(0, quarter)], y1s.at[h, part])

    @pl.when(holder)
    def _():
        for e in (1, 2, 3):
            for part in range(2):
                sent(piece(4 + x, hown, 0), xs_s.at[e, part])
        for e in range(4):
            for m in range(4):
                sent(piece(4 + x, hown, 0), y2s.at[e, m // 2, m % 2])

    for h in range(2):
        away = lax.rem(y + NY - 2 * k - h + NY, NY)

        @pl.when(jnp.logical_or(away == 1, away == 3))
        def _():
            for e in range(4):
                sent(piece(4 + x, h, 0), y3s.at[e, h])

    for j in range(4):

        @pl.when(4 * k + j != z)
        def _():
            sent(bsend.at[j], bs.at[j])

    @pl.when(k == home)
    def _():
        for zq in range(NZ):
            sent(bfull.at[zq], rel_s.at[zq])

    def drain(i, _):
        for e in (1, 2, 3):
            sent(csend.at[e - 1, i], cs.at[e - 1, i])
        for h in range(2):
            @pl.when(i != z)
            def _():
                sent(zsend.at[h, i], zs.at[h, i])

        return 0

    lax.fori_loop(0, NZ, drain, 0)

    piece_h = rows.at[x, k, :, pl.ds(0, half)]
    for h in range(2):

        @pl.when(x != y)
        def _():
            sent(piece_h, ts.at[h])

        for d in range(1, NZ):
            sent(piece_h, ccs.at[h, d])
            sent(piece_h, rs.at[h, d])

        @pl.when(k != home)
        def _():
            sent(piece_h, ccs.at[h, 0])

    for d in range(1, NZ):
        sent(ls.at[:, 0], l1s.at[d])
    for d in range(1, NY):
        sent(lz.at[0], l2s.at[d])
        sent(hsend.at[d - 1], hs.at[d])


def body(hidden_in, down_weight, keep_mask):
    ntok, kb = hidden_in.shape
    nb = down_weight.shape[0]
    scaling = 2.0 / (ntok * lax.axis_size("tok"))
    dma = pltpu.SemaphoreType.DMA
    hessian, rows = pl.pallas_call(
        lambda *refs: kernel(scaling, *refs),
        out_shape=(
            jax.ShapeDtypeStruct((nb, 4 * nb), F32),
            jax.ShapeDtypeStruct((NY, NZ, 8, nb), BF),
        ),
        in_specs=[pl.BlockSpec(memory_space=pl.ANY)] * 3,
        out_specs=(pl.BlockSpec(memory_space=pltpu.VMEM),) * 2,
        scratch_shapes=[
            pltpu.VMEM((ntok, kb), BF),
            pltpu.VMEM((4, nb, kb), BF),
            pltpu.VMEM((4, nb, kb), jnp.int32),
            pltpu.VMEM((4, nb, kb), BF),
            pltpu.VMEM((NZ, nb, kb), BF),
            pltpu.VMEM((8, ntok, kb), BF),
            pltpu.VMEM((3, NZ, nb, ntok), BF),
            pltpu.VMEM((2, NZ, nb, ntok), BF),
            pltpu.VMEM((NZ, nb, ntok), BF),
            pltpu.VMEM((NZ, nb, ntok), F32),
            pltpu.VMEM((2, NZ, nb, ntok // 2), BF),
            pltpu.VMEM((2, NZ, nb, ntok // 2), BF),
            pltpu.VMEM((2, nb, ntok // 2), F32),
            pltpu.VMEM((nb, ntok), BF),
            pltpu.VMEM((NX, 2, nb, ntok), BF),
            pltpu.VMEM((2, 4 * nb, ntok), BF),
            pltpu.VMEM((NY, NZ, 8, nb), BF),
            pltpu.VMEM((NY, NZ, 8, nb), BF),
            pltpu.VMEM((NY, NZ, 8, nb), BF),
            pltpu.VMEM((3, nb, 4 * nb), BF),
            pltpu.VMEM((NY, nb, 4 * nb), BF),
            pltpu.VMEM((NY, nb, 4 * nb), F32),
            dma((10,)),
            dma((2, 2)), dma((4, 2)), dma((4, 2)), dma((4, 2)),
            dma((4, 2, 2)), dma((2, 4, 2)), dma((4, 2)),
            dma((4,)), dma((NZ,)), dma((NZ,)),
            dma((3, NZ)), dma((2, NZ)), dma((NZ,)),
            dma((2, NZ)), dma((2, NZ)),
            dma((2,)), dma((2,)),
            dma((2, 8)), dma((2, 8)), dma((2, 8)), dma((2, 2, 4)),
            dma((8,)), dma((8,)), dma((4,)), dma((4,)),
            dma((4,)), dma((4,)),
        ],
        compiler_params=pltpu.CompilerParams(
            collective_id=0, has_side_effects=True, vmem_limit_bytes=60 * 2**20
        ),
    )(hidden_in, down_weight, keep_mask)
    layer_out = rows.transpose(2, 0, 1, 3).reshape(8, NY * NZ * nb)
    return layer_out, hessian


def solution(mesh):
    in_specs = (P("tok", "col"), P("col", "tok"), P("col", "tok"))
    out_specs = (P(("tok", "col"), None), P("col", "tok"))
    return jax.shard_map(body, mesh=mesh, in_specs=in_specs, out_specs=out_specs, check_vma=False)
```

```python
import jax
import jax.numpy as jnp
from jax import lax
from jax.experimental import pallas as pl
from jax.experimental.pallas import tpu as pltpu
from jax.sharding import PartitionSpec as P

MESH = pl.DeviceIdType.MESH
NX, NY, NZ = 4, 4, 8
BF = jnp.bfloat16
F32 = jnp.float32


def dot_nt(left, right):
    return lax.dot_general(
        left, right, (((1,), (1,)), ((), ())), preferred_element_type=F32
    )


def kernel(
    scaling,
    hid, wgt, msk,
    hout, lout,
    hbuf, wbuf, mbuf, bsend, bfull, abuf, csend, crecv, nrecv, pbuf, qbuf, zsend, zrecv,
    lacc, lt, rows, cols, ls, lz, lrecv, hsend, hrecv, hacc,
    in_sem, y1s, y1r, xs_s, xs_r, y2s, y2r, y3s, bs, br, rel_s, cs, cr, nr, zs, zr,
    ts, tr, rs, rr, ccs, ccr, l1s, l1r, l2s, l2r, hs, hr,
):
    t = lax.axis_index("tok")
    c = lax.axis_index("col")
    x, k = t // 2, lax.rem(t, 2)
    y, z = c // NZ, lax.rem(c, NZ)
    home = z // 4
    ntok = hid.shape[0]
    half = ntok // 2
    kb = hid.shape[1]
    nb = wgt.shape[0]

    def dev(xx, kk, yy, zz):
        return (xx * 2 + kk, yy * NZ + zz)

    def remote(src, dst, ssem, rsem, to):
        return pltpu.make_async_remote_copy(
            src_ref=src, dst_ref=dst, send_sem=ssem, recv_sem=rsem,
            device_id=to, device_id_type=MESH,
        )

    me = dev(x, k, y, z)

    def arrived(dst, rsem):
        remote(dst, dst, rsem, rsem, me).wait_recv()

    def sent(src, ssem):
        remote(src, src, ssem, ssem, me).wait_send()

    bar = pltpu.get_barrier_semaphore()
    for f in range(1, 8):
        pl.semaphore_signal(bar, inc=1, device_id=(lax.rem(t + f, 8), c), device_id_type=MESH)
    for d in range(1, NY):
        pl.semaphore_signal(bar, inc=1, device_id=dev(x, k, lax.rem(y + d, NY), z), device_id_type=MESH)
    for d in range(1, NZ):
        for kk in range(2):
            pl.semaphore_signal(bar, inc=1, device_id=dev(x, kk, y, lax.rem(z + d, NZ)), device_id_type=MESH)

    @pl.when(x != y)
    def _():
        pl.semaphore_signal(bar, inc=1, device_id=dev(y, k, x, z), device_id_type=MESH)

    aslot = jnp.where(y == x, 4 + x, y)
    holder = y // 2 == k
    hown = jnp.where(holder, y - 2 * k, 0)

    def load_piece(h, own):
        rows_h = pl.ds(h * half, half)
        dst = abuf.at[aslot, rows_h] if own else hbuf.at[rows_h]
        return pltpu.make_async_copy(hid.at[rows_h], dst, in_sem.at[h])

    def load_weight(j):
        return (
            pltpu.make_async_copy(wgt.at[:, pl.ds(j * kb, kb)], wbuf.at[j], in_sem.at[2 + j]),
            pltpu.make_async_copy(msk.at[:, pl.ds(j * kb, kb)], mbuf.at[j], in_sem.at[6 + j]),
        )

    for h in range(2):

        @pl.when(y == 2 * k + h)
        def _():
            load_piece(h, True).start()

        @pl.when(y != 2 * k + h)
        def _():
            load_piece(h, False).start()

    for j in range(4):
        for copy in load_weight(j):
            copy.start()

    def prune(j, _):
        for copy in load_weight_at(j):
            copy.wait()
        bsend[j] = wbuf[j] * mbuf[j].astype(BF)
        return 0

    def load_weight_at(j):
        return (
            pltpu.make_async_copy(wgt.at[:, pl.ds(0, kb)], wbuf.at[j], in_sem.at[2 + j]),
            pltpu.make_async_copy(msk.at[:, pl.ds(0, kb)], mbuf.at[j], in_sem.at[6 + j]),
        )

    lax.fori_loop(0, 4, prune, 0)

    pl.semaphore_wait(bar, jnp.where(x == y, 24, 25))

    quarter = half // 2

    for h in range(2):

        @pl.when(y == 2 * k + h)
        def _():
            load_piece(h, True).wait()

        @pl.when(y != 2 * k + h)
        def _():
            load_piece(h, False).wait()
    for part in range(2):
        for h in range(2):

            @pl.when(y != 2 * k + h)
            def _():
                rows_p = pl.ds(h * half + part * quarter, quarter)
                remote(
                    hbuf.at[rows_p], abuf.at[aslot, rows_p],
                    y1s.at[h, part], y1r.at[y, part], dev(x, k, 2 * k + h, z),
                ).start()

    def zpart(i):
        i = jnp.int32(i)
        return lax.rem(z + jnp.where(lax.rem(i, 2) == 1, (i + 1) // 2, NZ - i // 2), NZ)

    def place(d):
        return jnp.where(d == 0, 0, jnp.where(d <= 4, 2 * d - 1, 2 * (NZ - d)))

    def hand_out(i, _):
        zt = zpart(i)

        @pl.when(zt // 4 == k)
        def _():
            j = lax.rem(zt, 4)

            @pl.when(zt == z)
            def _():
                bfull[0] = bsend[j]

            @pl.when(zt != z)
            def _():
                slot = place(lax.rem(z + NZ - zt, NZ))
                remote(bsend.at[j], bfull.at[slot], bs.at[j], br.at[slot], dev(x, k, y, zt)).start()

        return 0

    lax.fori_loop(0, NZ, hand_out, 0)

    order = (2, 1, 3, 0)

    def piece(slot, h, part=None):
        if part is None:
            return abuf.at[slot, pl.ds(h * half, half)]
        return abuf.at[slot, pl.ds(h * half + part * quarter, quarter)]

    def handed(e, h, part, ssem, up):
        slot = 4 + lax.rem(x + e, NX)
        return remote(
            piece(slot, h, part), piece(slot, h, part), ssem, y2r.at[h, e, part],
            dev(x, k, lax.rem(y + (1 if up else NY - 1), NY), z),
        )

    @pl.when(holder)
    def _():
        for part in range(2):
            for e in (2, 1, 3):
                ys = lax.rem(x + NX - e, NX)

                @pl.when(ys != y)
                def _():
                    arrived(piece(ys, hown, part), y1r.at[ys, part])

                remote(
                    piece(ys, hown, part), piece(4 + x, hown, part),
                    xs_s.at[e, part], xs_r.at[x, part], dev(ys, k, y, z),
                ).start()
        for e in order:
            xe = lax.rem(x + e, NX)
            for part in range(2):
                if e:
                    arrived(piece(4 + xe, hown, part), xs_r.at[xe, part])
                else:

                    @pl.when(x != y)
                    def _():
                        arrived(piece(4 + x, hown, part), y1r.at[x, part])

                for up in (part == 0, part == 1):
                    handed(e, hown, part, y2s.at[e, part, int(up)], up).start()

    def relay_tokens(e):
        for h in range(2):
            away = lax.rem(y + NY - 2 * k - h + NY, NY)

            @pl.when(away == 1)
            def _():
                arrived(piece(4 + lax.rem(x + e, NX), h, 0), y2r.at[h, e, 0])
                handed(e, h, 0, y3s.at[e, h], True).start()

            @pl.when(away == 3)
            def _():
                arrived(piece(4 + lax.rem(x + e, NX), h, 1), y2r.at[h, e, 1])
                handed(e, h, 1, y3s.at[e, h], False).start()

    def tokens_here(e):
        for h in range(2):
            away = lax.rem(y + NY - 2 * k - h + NY, NY)

            @pl.when(away >= 2)
            def _():
                arrived(piece(4 + lax.rem(x + e, NX), h, 0), y2r.at[h, e, 0])

            @pl.when(jnp.logical_or(away == 1, away == 2))
            def _():
                arrived(piece(4 + lax.rem(x + e, NX), h, 1), y2r.at[h, e, 1])

    def relay_weights(i, _):
        @pl.when(jnp.logical_or(k != home, i > 0))
        def _():
            arrived(bfull.at[i], br.at[i])

        @pl.when(k == home)
        def _():
            remote(bfull.at[i], bfull.at[i], rel_s.at[i], br.at[i], dev(x, 1 - k, y, z)).start()

        return 0

    def product(e, lo, hi):
        left = bfull[lo:hi].reshape((hi - lo) * nb, kb)
        return dot_nt(left, abuf[4 + lax.rem(x + e, NX)]).reshape(hi - lo, nb, ntok)

    via_up, via_down = (0, 2, 4), (1, 3, 5)

    def products(e, lo, hi, order=None):
        qbuf[lo:hi] = product(e, lo, hi)
        for i in order or range(lo, hi):
            src, ssem = csend.at[e - 1, i], cs.at[e - 1, i]
            if e == 2:
                csend[1, i] = qbuf[i].astype(BF)
                to = lax.rem(x + (1 if i in via_up else NX - 1 if i in via_down else 2), NX)
                remote(src, nrecv.at[i], ssem, nr.at[i], dev(to, k, y, z)).start()
                continue
            if i in (via_up if e == 1 else via_down):
                arrived(nrecv.at[i], nr.at[i])
                csend[e - 1, i] = (qbuf[i] + nrecv[i].astype(F32)).astype(BF)
            else:
                csend[e - 1, i] = qbuf[i].astype(BF)
            remote(
                src, crecv.at[e // 2, i], ssem, cr.at[e // 2, i], dev(lax.rem(x + e, NX), k, y, z)
            ).start()

    def weights(lo, hi):
        lax.fori_loop(lo, hi, relay_weights, 0)

    relay_tokens(2)
    weights(0, 3)
    relay_tokens(1)
    tokens_here(2)
    products(2, 0, 3)
    relay_tokens(3)
    weights(3, 5)
    products(2, 3, 5)
    relay_tokens(0)
    weights(5, 7)
    products(2, 5, 7)
    tokens_here(1)
    products(1, 0, 7, order=(1, 2, 3, 4, 5, 6, 0))
    tokens_here(3)
    products(3, 0, 7, order=(1, 2, 3, 4, 5, 6, 0))
    tokens_here(0)
    pbuf[0:7] = product(0, 0, 7)

    def reduce_x(i):
        for side in range(2):
            arrived(crecv.at[side, i], cr.at[side, i])
        acc = pbuf[i] + crecv[0, i].astype(F32) + crecv[1, i].astype(F32)
        if i not in via_up + via_down:
            arrived(nrecv.at[i], nr.at[i])
            acc = acc + nrecv[i].astype(F32)
        return acc

    def reduce_send(i):
        zq = zpart(i)
        acc = reduce_x(i).astype(BF)
        for h in range(2):
            zsend[h, zq] = acc[:, h * half : (h + 1) * half]
            remote(
                zsend.at[h, zq], zrecv.at[h, z], zs.at[h, zq], zr.at[h, z], dev(x, k, y, zq)
            ).start()

    reduce_send(1)
    weights(7, 8)
    products(2, 7, 8)
    products(3, 7, 8)
    products(1, 7, 8)
    pbuf[7] = product(0, 7, 8)[0]
    for i in (2, 3, 4, 5, 6, 7):
        reduce_send(i)
    acc = reduce_x(0)
    for h in range(2):
        lacc[h] = acc[:, h * half : (h + 1) * half]

    def reduce_z(h):
        lanes = pl.ds(h * half, half)

        def step(d, _):
            zq = lax.rem(z + d, NZ)
            arrived(zrecv.at[h, zq], zr.at[h, zq])
            lacc[h] += zrecv[h, zq].astype(F32)
            return 0

        lax.fori_loop(1, NZ, step, 0)
        lt[:, lanes] = lacc[h].astype(BF)

        @pl.when(x != y)
        def _():
            remote(lt.at[:, lanes], rows.at[y, k, :, lanes], ts.at[h], tr.at[h], dev(y, k, x, z)).start()

        @pl.when(x == y)
        def _():
            rows[x, k, :, lanes] = lt[:, lanes]

    zrow = lax.rem(z, 4) * nb

    def tok_send(f, h):
        t2 = lax.rem(t + f, 8)
        mine = rows.at[x, k, :, pl.ds(h * half, half)]
        return remote(mine, mine, rs.at[h, f], rr.at[h, t], (t2, c))

    def col_send(d, h):
        lanes = pl.ds(h * half, half)
        return remote(
            rows.at[x, k, :, lanes], cols.at[k, pl.ds(zrow, nb), lanes],
            ccs.at[h, d], ccr.at[h, k, lax.rem(z, 4)],
            dev(x, home, y, lax.rem(z + d, NZ)),
        )

    def spread(h):
        lanes = pl.ds(h * half, half)

        @pl.when(x != y)
        def _():
            arrived(rows.at[x, k, :, lanes], tr.at[h])

        for d in (4, 3, 5, 2, 6, 1, 7):
            col_send(d, h).start()

        @pl.when(k != home)
        def _():
            col_send(0, h).start()

        @pl.when(k == home)
        def _():
            cols[k, pl.ds(zrow, nb), lanes] = rows[x, k, :, lanes]

        for f in (4, 5, 2, 3, 6, 7, 1):
            tok_send(f, h).start()

    reduce_z(0)
    reduce_z(1)

    ident = (
        lax.broadcasted_iota(jnp.int32, (ntok, ntok), 0)
        == lax.broadcasted_iota(jnp.int32, (ntok, ntok), 1)
    ).astype(F32).astype(BF)
    ls[...] = dot_nt(ident, lt[...]).reshape(NY, NZ, 8, nb).astype(BF)
    for d in range(1, NZ):
        z2 = lax.rem(z + d, NZ)
        remote(ls.at[:, z2], lz.at[:, z], l1s.at[d], l1r.at[z], dev(x, k, y, z2)).start()
    lz[:, z] = ls[:, z]

    spread(0)
    spread(1)

    for d in range(1, NZ):
        zq = lax.rem(z + d, NZ)
        arrived(lz.at[:, zq], l1r.at[zq])
    for d in range(1, NY):
        y2 = lax.rem(y + d, NY)
        remote(lz.at[y2], lrecv.at[y], l2s.at[d], l2r.at[y], dev(x, k, y2, z)).start()
    lrecv[y] = lz[y]

    for f in range(1, 8):
        t2 = lax.rem(t + f, 8)
        for h in range(2):
            arrived(rows.at[t2 // 2, lax.rem(t2, 2), :, pl.ds(h * half, half)], rr.at[h, t2])
    for kk in range(2):
        for j in range(4):
            @pl.when(jnp.logical_or(4 * k + j != z, k != kk))
            def _():
                for h in range(2):
                    arrived(cols.at[kk, pl.ds(j * nb, nb), pl.ds(h * half, half)], ccr.at[h, kk, j])

    part = sum(dot_nt(rows[:, kk].reshape(NY * nb, ntok), cols[kk]) for kk in range(2))
    hacc[...] = (part * scaling).reshape(NY, nb, NY * nb)
    for e in (2, 1, 3):
        y2 = lax.rem(y + e, NY)
        hsend[e - 1] = hacc[y2].astype(BF)
        remote(hsend.at[e - 1], hrecv.at[y], hs.at[e], hr.at[y], dev(x, k, y2, z)).start()
    hout[...] = hacc[y]
    for h in range(2):

        @pl.when(y != 2 * k + h)
        def _():
            for part in range(2):
                sent(hbuf.at[pl.ds(0, quarter)], y1s.at[h, part])

    @pl.when(holder)
    def _():
        for e in (1, 2, 3):
            for part in range(2):
                sent(piece(4 + x, hown, 0), xs_s.at[e, part])
        for e in range(4):
            for m in range(4):
                sent(piece(4 + x, hown, 0), y2s.at[e, m // 2, m % 2])

    for h in range(2):
        away = lax.rem(y + NY - 2 * k - h + NY, NY)

        @pl.when(jnp.logical_or(away == 1, away == 3))
        def _():
            for e in range(4):
                sent(piece(4 + x, h, 0), y3s.at[e, h])

    for j in range(4):

        @pl.when(4 * k + j != z)
        def _():
            sent(bsend.at[j], bs.at[j])

    @pl.when(k == home)
    def _():
        for zq in range(NZ):
            sent(bfull.at[zq], rel_s.at[zq])

    def drain(i, _):
        for e in (1, 2, 3):
            sent(csend.at[e - 1, i], cs.at[e - 1, i])
        for h in range(2):
            @pl.when(i != z)
            def _():
                sent(zsend.at[h, i], zs.at[h, i])

        return 0

    lax.fori_loop(0, NZ, drain, 0)

    piece_h = rows.at[x, k, :, pl.ds(0, half)]
    for h in range(2):

        @pl.when(x != y)
        def _():
            sent(piece_h, ts.at[h])

        for d in range(1, NZ):
            sent(piece_h, ccs.at[h, d])
            sent(piece_h, rs.at[h, d])

        @pl.when(k != home)
        def _():
            sent(piece_h, ccs.at[h, 0])

    for d in range(1, NZ):
        sent(ls.at[:, 0], l1s.at[d])

    for e in (1, 3, 2):
        ys = lax.rem(y + e, NY)
        arrived(hrecv.at[ys], hr.at[ys])
        hout[...] += hrecv[ys].astype(F32)

    for d in range(1, NY):
        ys = lax.rem(y + d, NY)
        arrived(lrecv.at[ys], l2r.at[ys])
    for ys in range(NY):
        for zq in range(NZ):
            at = (ys * NZ + zq) * nb
            lout[:, at : at + nb] = lrecv[ys, zq]
    for d in range(1, NY):
        sent(lz.at[0], l2s.at[d])
        sent(hsend.at[d - 1], hs.at[d])


def body(hidden_in, down_weight, keep_mask):
    ntok, kb = hidden_in.shape
    nb = down_weight.shape[0]
    scaling = 2.0 / (ntok * lax.axis_size("tok"))
    dma = pltpu.SemaphoreType.DMA
    hessian, layer_out = pl.pallas_call(
        lambda *refs: kernel(scaling, *refs),
        out_shape=(
            jax.ShapeDtypeStruct((nb, 4 * nb), F32),
            jax.ShapeDtypeStruct((8, NY * NZ * nb), BF),
        ),
        in_specs=[pl.BlockSpec(memory_space=pl.ANY)] * 3,
        out_specs=(pl.BlockSpec(memory_space=pltpu.VMEM),) * 2,
        scratch_shapes=[
            pltpu.VMEM((ntok, kb), BF),
            pltpu.VMEM((4, nb, kb), BF),
            pltpu.VMEM((4, nb, kb), jnp.int32),
            pltpu.VMEM((4, nb, kb), BF),
            pltpu.VMEM((NZ, nb, kb), BF),
            pltpu.VMEM((8, ntok, kb), BF),
            pltpu.VMEM((3, NZ, nb, ntok), BF),
            pltpu.VMEM((2, NZ, nb, ntok), BF),
            pltpu.VMEM((NZ, nb, ntok), BF),
            pltpu.VMEM((NZ, nb, ntok), F32),
            pltpu.VMEM((NZ, nb, ntok), F32),
            pltpu.VMEM((2, NZ, nb, ntok // 2), BF),
            pltpu.VMEM((2, NZ, nb, ntok // 2), BF),
            pltpu.VMEM((2, nb, ntok // 2), F32),
            pltpu.VMEM((nb, ntok), BF),
            pltpu.VMEM((NX, 2, nb, ntok), BF),
            pltpu.VMEM((2, 4 * nb, ntok), BF),
            pltpu.VMEM((NY, NZ, 8, nb), BF),
            pltpu.VMEM((NY, NZ, 8, nb), BF),
            pltpu.VMEM((NY, NZ, 8, nb), BF),
            pltpu.VMEM((3, nb, 4 * nb), BF),
            pltpu.VMEM((NY, nb, 4 * nb), BF),
            pltpu.VMEM((NY, nb, 4 * nb), F32),
            dma((10,)),
            dma((2, 2)), dma((4, 2)), dma((4, 2)), dma((4, 2)),
            dma((4, 2, 2)), dma((2, 4, 2)), dma((4, 2)),
            dma((4,)), dma((NZ,)), dma((NZ,)),
            dma((3, NZ)), dma((2, NZ)), dma((NZ,)),
            dma((2, NZ)), dma((2, NZ)),
            dma((2,)), dma((2,)),
            dma((2, 8)), dma((2, 8)), dma((2, 8)), dma((2, 2, 4)),
            dma((8,)), dma((8,)), dma((4,)), dma((4,)),
            dma((4,)), dma((4,)),
        ],
        compiler_params=pltpu.CompilerParams(
            collective_id=0, has_side_effects=True, vmem_limit_bytes=60 * 2**20
        ),
    )(hidden_in, down_weight, keep_mask)
    return layer_out, hessian


def solution(mesh):
    in_specs = (P("tok", "col"), P("col", "tok"), P("col", "tok"))
    out_specs = (P(("tok", "col"), None), P("col", "tok"))
    return jax.shard_map(body, mesh=mesh, in_specs=in_specs, out_specs=out_specs, check_vma=False)
```

```python
import jax
import jax.numpy as jnp
from jax import lax
from jax.experimental import pallas as pl
from jax.experimental.pallas import tpu as pltpu
from jax.sharding import PartitionSpec as P

MESH = pl.DeviceIdType.MESH
NX, NY, NZ = 4, 4, 8
BF = jnp.bfloat16
F32 = jnp.float32


def dot_nt(left, right):
    return lax.dot_general(
        left, right, (((1,), (1,)), ((), ())), preferred_element_type=F32
    )


def kernel(
    scaling,
    hid, wgt, msk,
    hout, lout,
    hbuf, wbuf, mbuf, bsend, bfull, abuf, csend, crecv, nrecv, pbuf, qbuf, zsend, zrecv,
    lacc, lt, rows, cols, ls, lz, lrecv, hsend, hrecv, hacc,
    in_sem, y1s, y1r, xs_s, xs_r, y2s, y2r, y3s, bs, br, rel_s, cs, cr, nr, zs, zr,
    ts, tr, rs, rr, ccs, ccr, l1s, l1r, l2s, l2r, hs, hr,
):
    t = lax.axis_index("tok")
    c = lax.axis_index("col")
    x, k = t // 2, lax.rem(t, 2)
    y, z = c // NZ, lax.rem(c, NZ)
    home = z // 4
    ntok = hid.shape[0]
    half = ntok // 2
    kb = hid.shape[1]
    nb = wgt.shape[0]

    def dev(xx, kk, yy, zz):
        return (xx * 2 + kk, yy * NZ + zz)

    def remote(src, dst, ssem, rsem, to):
        return pltpu.make_async_remote_copy(
            src_ref=src, dst_ref=dst, send_sem=ssem, recv_sem=rsem,
            device_id=to, device_id_type=MESH,
        )

    me = dev(x, k, y, z)

    def arrived(dst, rsem):
        remote(dst, dst, rsem, rsem, me).wait_recv()

    def sent(src, ssem):
        remote(src, src, ssem, ssem, me).wait_send()

    bar = pltpu.get_barrier_semaphore()
    for f in range(1, 8):
        pl.semaphore_signal(bar, inc=1, device_id=(lax.rem(t + f, 8), c), device_id_type=MESH)
    for d in range(1, NY):
        pl.semaphore_signal(bar, inc=1, device_id=dev(x, k, lax.rem(y + d, NY), z), device_id_type=MESH)
    for d in range(1, NZ):
        for kk in range(2):
            pl.semaphore_signal(bar, inc=1, device_id=dev(x, kk, y, lax.rem(z + d, NZ)), device_id_type=MESH)

    @pl.when(x != y)
    def _():
        pl.semaphore_signal(bar, inc=1, device_id=dev(y, k, x, z), device_id_type=MESH)

    aslot = jnp.where(y == x, 4 + x, y)
    holder = y // 2 == k
    hown = jnp.where(holder, y - 2 * k, 0)

    def load_piece(h, own):
        rows_h = pl.ds(h * half, half)
        dst = abuf.at[aslot, rows_h] if own else hbuf.at[rows_h]
        return pltpu.make_async_copy(hid.at[rows_h], dst, in_sem.at[h])

    def load_weight(j):
        return (
            pltpu.make_async_copy(wgt.at[:, pl.ds(j * kb, kb)], wbuf.at[j], in_sem.at[2 + j]),
            pltpu.make_async_copy(msk.at[:, pl.ds(j * kb, kb)], mbuf.at[j], in_sem.at[6 + j]),
        )

    for h in range(2):

        @pl.when(y == 2 * k + h)
        def _():
            load_piece(h, True).start()

        @pl.when(y != 2 * k + h)
        def _():
            load_piece(h, False).start()

    for j in range(4):
        for copy in load_weight(j):
            copy.start()

    def prune(j, _):
        for copy in load_weight_at(j):
            copy.wait()
        bsend[j] = wbuf[j] * mbuf[j].astype(BF)
        return 0

    def load_weight_at(j):
        return (
            pltpu.make_async_copy(wgt.at[:, pl.ds(0, kb)], wbuf.at[j], in_sem.at[2 + j]),
            pltpu.make_async_copy(msk.at[:, pl.ds(0, kb)], mbuf.at[j], in_sem.at[6 + j]),
        )

    pl.semaphore_wait(bar, jnp.where(x == y, 24, 25))

    quarter = half // 2

    for h in range(2):

        @pl.when(y == 2 * k + h)
        def _():
            load_piece(h, True).wait()

        @pl.when(y != 2 * k + h)
        def _():
            load_piece(h, False).wait()
    for part in range(2):
        for h in range(2):

            @pl.when(y != 2 * k + h)
            def _():
                rows_p = pl.ds(h * half + part * quarter, quarter)
                remote(
                    hbuf.at[rows_p], abuf.at[aslot, rows_p],
                    y1s.at[h, part], y1r.at[y, part], dev(x, k, 2 * k + h, z),
                ).start()

    def zpart(i):
        i = jnp.int32(i)
        return lax.rem(z + jnp.where(lax.rem(i, 2) == 1, (i + 1) // 2, NZ - i // 2), NZ)

    def place(d):
        return jnp.where(d == 0, 0, jnp.where(d <= 4, 2 * d - 1, 2 * (NZ - d)))

    def hand_out(i, _):
        zt = zpart(i)

        @pl.when(zt // 4 == k)
        def _():
            j = lax.rem(zt, 4)

            @pl.when(zt == z)
            def _():
                bfull[0] = bsend[j]

            @pl.when(zt != z)
            def _():
                slot = place(lax.rem(z + NZ - zt, NZ))
                remote(bsend.at[j], bfull.at[slot], bs.at[j], br.at[slot], dev(x, k, y, zt)).start()

        return 0

    lax.fori_loop(0, 4, prune, 0)
    lax.fori_loop(0, NZ, hand_out, 0)

    order = (2, 1, 3, 0)

    def piece(slot, h, part=None):
        if part is None:
            return abuf.at[slot, pl.ds(h * half, half)]
        return abuf.at[slot, pl.ds(h * half + part * quarter, quarter)]

    def handed(e, h, part, ssem, up):
        slot = 4 + lax.rem(x + e, NX)
        return remote(
            piece(slot, h, part), piece(slot, h, part), ssem, y2r.at[h, e, part],
            dev(x, k, lax.rem(y + (1 if up else NY - 1), NY), z),
        )

    @pl.when(holder)
    def _():
        for part in range(2):
            for e in (2, 1, 3):
                ys = lax.rem(x + NX - e, NX)

                @pl.when(ys != y)
                def _():
                    arrived(piece(ys, hown, part), y1r.at[ys, part])

                remote(
                    piece(ys, hown, part), piece(4 + x, hown, part),
                    xs_s.at[e, part], xs_r.at[x, part], dev(ys, k, y, z),
                ).start()
        for e in order:
            xe = lax.rem(x + e, NX)
            for part in range(2):
                if e:
                    arrived(piece(4 + xe, hown, part), xs_r.at[xe, part])
                else:

                    @pl.when(x != y)
                    def _():
                        arrived(piece(4 + x, hown, part), y1r.at[x, part])

                for up in (part == 0, part == 1):
                    handed(e, hown, part, y2s.at[e, part, int(up)], up).start()

    def relay_tokens(e):
        for h in range(2):
            away = lax.rem(y + NY - 2 * k - h + NY, NY)

            @pl.when(away == 1)
            def _():
                arrived(piece(4 + lax.rem(x + e, NX), h, 0), y2r.at[h, e, 0])
                handed(e, h, 0, y3s.at[e, h], True).start()

            @pl.when(away == 3)
            def _():
                arrived(piece(4 + lax.rem(x + e, NX), h, 1), y2r.at[h, e, 1])
                handed(e, h, 1, y3s.at[e, h], False).start()

    def tokens_here(e):
        for h in range(2):
            away = lax.rem(y + NY - 2 * k - h + NY, NY)

            @pl.when(away >= 2)
            def _():
                arrived(piece(4 + lax.rem(x + e, NX), h, 0), y2r.at[h, e, 0])

            @pl.when(jnp.logical_or(away == 1, away == 2))
            def _():
                arrived(piece(4 + lax.rem(x + e, NX), h, 1), y2r.at[h, e, 1])

    def relay_weights(i, _):
        @pl.when(jnp.logical_or(k != home, i > 0))
        def _():
            arrived(bfull.at[i], br.at[i])

        @pl.when(k == home)
        def _():
            remote(bfull.at[i], bfull.at[i], rel_s.at[i], br.at[i], dev(x, 1 - k, y, z)).start()

        return 0

    def product(e, lo, hi):
        left = bfull[lo:hi].reshape((hi - lo) * nb, kb)
        return dot_nt(left, abuf[4 + lax.rem(x + e, NX)]).reshape(hi - lo, nb, ntok)

    via_up, via_down = (0, 2, 4), (1, 3, 5)

    def products(e, lo, hi, order=None):
        qbuf[lo:hi] = product(e, lo, hi)
        for i in order or range(lo, hi):
            src, ssem = csend.at[e - 1, i], cs.at[e - 1, i]
            if e == 2:
                csend[1, i] = qbuf[i].astype(BF)
                to = lax.rem(x + (1 if i in via_up else NX - 1 if i in via_down else 2), NX)
                remote(src, nrecv.at[i], ssem, nr.at[i], dev(to, k, y, z)).start()
                continue
            if i in (via_up if e == 1 else via_down):
                arrived(nrecv.at[i], nr.at[i])
                csend[e - 1, i] = (qbuf[i] + nrecv[i].astype(F32)).astype(BF)
            else:
                csend[e - 1, i] = qbuf[i].astype(BF)
            remote(
                src, crecv.at[e // 2, i], ssem, cr.at[e // 2, i], dev(lax.rem(x + e, NX), k, y, z)
            ).start()

    def weights(lo, hi):
        lax.fori_loop(lo, hi, relay_weights, 0)

    relay_tokens(2)
    weights(0, 3)
    relay_tokens(1)
    weights(3, 5)
    tokens_here(2)
    products(2, 0, 5)
    relay_tokens(3)
    relay_tokens(0)
    weights(5, 7)
    products(2, 5, 7)
    tokens_here(1)
    products(1, 0, 7, order=(1, 2, 3, 4, 5, 6, 0))
    tokens_here(3)
    products(3, 0, 7, order=(1, 2, 3, 4, 5, 6, 0))
    tokens_here(0)
    pbuf[0:7] = product(0, 0, 7)

    def reduce_x(i):
        for side in range(2):
            arrived(crecv.at[side, i], cr.at[side, i])
        acc = pbuf[i] + crecv[0, i].astype(F32) + crecv[1, i].astype(F32)
        if i not in via_up + via_down:
            arrived(nrecv.at[i], nr.at[i])
            acc = acc + nrecv[i].astype(F32)
        return acc

    def reduce_send(i):
        zq = zpart(i)
        acc = reduce_x(i).astype(BF)
        for h in range(2):
            zsend[h, zq] = acc[:, h * half : (h + 1) * half]
            remote(
                zsend.at[h, zq], zrecv.at[h, z], zs.at[h, zq], zr.at[h, z], dev(x, k, y, zq)
            ).start()

    reduce_send(1)
    weights(7, 8)
    products(2, 7, 8)
    products(3, 7, 8)
    products(1, 7, 8)
    pbuf[7] = product(0, 7, 8)[0]
    for i in (2, 3, 4, 5, 6, 7):
        reduce_send(i)
    acc = reduce_x(0)
    for h in range(2):
        lacc[h] = acc[:, h * half : (h + 1) * half]

    def reduce_z(h):
        lanes = pl.ds(h * half, half)

        def step(d, _):
            zq = lax.rem(z + d, NZ)
            arrived(zrecv.at[h, zq], zr.at[h, zq])
            lacc[h] += zrecv[h, zq].astype(F32)
            return 0

        lax.fori_loop(1, NZ, step, 0)
        lt[:, lanes] = lacc[h].astype(BF)

        @pl.when(x != y)
        def _():
            remote(lt.at[:, lanes], rows.at[y, k, :, lanes], ts.at[h], tr.at[h], dev(y, k, x, z)).start()

        @pl.when(x == y)
        def _():
            rows[x, k, :, lanes] = lt[:, lanes]

    zrow = lax.rem(z, 4) * nb

    def tok_send(f, h):
        t2 = lax.rem(t + f, 8)
        mine = rows.at[x, k, :, pl.ds(h * half, half)]
        return remote(mine, mine, rs.at[h, f], rr.at[h, t], (t2, c))

    def col_send(d, h):
        lanes = pl.ds(h * half, half)
        return remote(
            rows.at[x, k, :, lanes], cols.at[k, pl.ds(zrow, nb), lanes],
            ccs.at[h, d], ccr.at[h, k, lax.rem(z, 4)],
            dev(x, home, y, lax.rem(z + d, NZ)),
        )

    def spread(h):
        lanes = pl.ds(h * half, half)

        @pl.when(x != y)
        def _():
            arrived(rows.at[x, k, :, lanes], tr.at[h])

        for d in (4, 3, 5, 2, 6, 1, 7):
            col_send(d, h).start()

        @pl.when(k != home)
        def _():
            col_send(0, h).start()

        @pl.when(k == home)
        def _():
            cols[k, pl.ds(zrow, nb), lanes] = rows[x, k, :, lanes]

        for f in (4, 5, 2, 3, 6, 7, 1):
            tok_send(f, h).start()

    reduce_z(0)
    reduce_z(1)

    ident = (
        lax.broadcasted_iota(jnp.int32, (ntok, ntok), 0)
        == lax.broadcasted_iota(jnp.int32, (ntok, ntok), 1)
    ).astype(F32).astype(BF)
    ls[...] = dot_nt(ident, lt[...]).reshape(NY, NZ, 8, nb).astype(BF)
    for d in range(1, NZ):
        z2 = lax.rem(z + d, NZ)
        remote(ls.at[:, z2], lz.at[:, z], l1s.at[d], l1r.at[z], dev(x, k, y, z2)).start()
    lz[:, z] = ls[:, z]

    spread(0)
    spread(1)

    for d in range(1, NZ):
        zq = lax.rem(z + d, NZ)
        arrived(lz.at[:, zq], l1r.at[zq])
    for d in range(1, NY):
        y2 = lax.rem(y + d, NY)
        remote(lz.at[y2], lrecv.at[y], l2s.at[d], l2r.at[y], dev(x, k, y2, z)).start()
    lrecv[y] = lz[y]

    for f in range(1, 8):
        t2 = lax.rem(t + f, 8)
        for h in range(2):
            arrived(rows.at[t2 // 2, lax.rem(t2, 2), :, pl.ds(h * half, half)], rr.at[h, t2])
    for kk in range(2):
        for j in range(4):
            @pl.when(jnp.logical_or(4 * k + j != z, k != kk))
            def _():
                for h in range(2):
                    arrived(cols.at[kk, pl.ds(j * nb, nb), pl.ds(h * half, half)], ccr.at[h, kk, j])

    part = sum(dot_nt(rows[:, kk].reshape(NY * nb, ntok), cols[kk]) for kk in range(2))
    hacc[...] = (part * scaling).reshape(NY, nb, NY * nb)
    for e in (2, 1, 3):
        y2 = lax.rem(y + e, NY)
        hsend[e - 1] = hacc[y2].astype(BF)
        remote(hsend.at[e - 1], hrecv.at[y], hs.at[e], hr.at[y], dev(x, k, y2, z)).start()
    hout[...] = hacc[y]
    for h in range(2):

        @pl.when(y != 2 * k + h)
        def _():
            for part in range(2):
                sent(hbuf.at[pl.ds(0, quarter)], y1s.at[h, part])

    @pl.when(holder)
    def _():
        for e in (1, 2, 3):
            for part in range(2):
                sent(piece(4 + x, hown, 0), xs_s.at[e, part])
        for e in range(4):
            for m in range(4):
                sent(piece(4 + x, hown, 0), y2s.at[e, m // 2, m % 2])

    for h in range(2):
        away = lax.rem(y + NY - 2 * k - h + NY, NY)

        @pl.when(jnp.logical_or(away == 1, away == 3))
        def _():
            for e in range(4):
                sent(piece(4 + x, h, 0), y3s.at[e, h])

    for j in range(4):

        @pl.when(4 * k + j != z)
        def _():
            sent(bsend.at[j], bs.at[j])

    @pl.when(k == home)
    def _():
        for zq in range(NZ):
            sent(bfull.at[zq], rel_s.at[zq])

    def drain(i, _):
        for e in (1, 2, 3):
            sent(csend.at[e - 1, i], cs.at[e - 1, i])
        for h in range(2):
            @pl.when(i != z)
            def _():
                sent(zsend.at[h, i], zs.at[h, i])

        return 0

    lax.fori_loop(0, NZ, drain, 0)

    piece_h = rows.at[x, k, :, pl.ds(0, half)]
    for h in range(2):

        @pl.when(x != y)
        def _():
            sent(piece_h, ts.at[h])

        for d in range(1, NZ):
            sent(piece_h, ccs.at[h, d])
            sent(piece_h, rs.at[h, d])

        @pl.when(k != home)
        def _():
            sent(piece_h, ccs.at[h, 0])

    for d in range(1, NZ):
        sent(ls.at[:, 0], l1s.at[d])

    for e in (1, 3, 2):
        ys = lax.rem(y + e, NY)
        arrived(hrecv.at[ys], hr.at[ys])
        hout[...] += hrecv[ys].astype(F32)

    for d in range(1, NY):
        ys = lax.rem(y + d, NY)
        arrived(lrecv.at[ys], l2r.at[ys])
    for ys in range(NY):
        for zq in range(NZ):
            at = (ys * NZ + zq) * nb
            lout[:, at : at + nb] = lrecv[ys, zq]
    for d in range(1, NY):
        sent(lz.at[0], l2s.at[d])
        sent(hsend.at[d - 1], hs.at[d])


def body(hidden_in, down_weight, keep_mask):
    ntok, kb = hidden_in.shape
    nb = down_weight.shape[0]
    scaling = 2.0 / (ntok * lax.axis_size("tok"))
    dma = pltpu.SemaphoreType.DMA
    hessian, layer_out = pl.pallas_call(
        lambda *refs: kernel(scaling, *refs),
        out_shape=(
            jax.ShapeDtypeStruct((nb, 4 * nb), F32),
            jax.ShapeDtypeStruct((8, NY * NZ * nb), BF),
        ),
        in_specs=[pl.BlockSpec(memory_space=pl.ANY)] * 3,
        out_specs=(pl.BlockSpec(memory_space=pltpu.VMEM),) * 2,
        scratch_shapes=[
            pltpu.VMEM((ntok, kb), BF),
            pltpu.VMEM((4, nb, kb), BF),
            pltpu.VMEM((4, nb, kb), jnp.int32),
            pltpu.VMEM((4, nb, kb), BF),
            pltpu.VMEM((NZ, nb, kb), BF),
            pltpu.VMEM((8, ntok, kb), BF),
            pltpu.VMEM((3, NZ, nb, ntok), BF),
            pltpu.VMEM((2, NZ, nb, ntok), BF),
            pltpu.VMEM((NZ, nb, ntok), BF),
            pltpu.VMEM((NZ, nb, ntok), F32),
            pltpu.VMEM((NZ, nb, ntok), F32),
            pltpu.VMEM((2, NZ, nb, ntok // 2), BF),
            pltpu.VMEM((2, NZ, nb, ntok // 2), BF),
            pltpu.VMEM((2, nb, ntok // 2), F32),
            pltpu.VMEM((nb, ntok), BF),
            pltpu.VMEM((NX, 2, nb, ntok), BF),
            pltpu.VMEM((2, 4 * nb, ntok), BF),
            pltpu.VMEM((NY, NZ, 8, nb), BF),
            pltpu.VMEM((NY, NZ, 8, nb), BF),
            pltpu.VMEM((NY, NZ, 8, nb), BF),
            pltpu.VMEM((3, nb, 4 * nb), BF),
            pltpu.VMEM((NY, nb, 4 * nb), BF),
            pltpu.VMEM((NY, nb, 4 * nb), F32),
            dma((10,)),
            dma((2, 2)), dma((4, 2)), dma((4, 2)), dma((4, 2)),
            dma((4, 2, 2)), dma((2, 4, 2)), dma((4, 2)),
            dma((4,)), dma((NZ,)), dma((NZ,)),
            dma((3, NZ)), dma((2, NZ)), dma((NZ,)),
            dma((2, NZ)), dma((2, NZ)),
            dma((2,)), dma((2,)),
            dma((2, 8)), dma((2, 8)), dma((2, 8)), dma((2, 2, 4)),
            dma((8,)), dma((8,)), dma((4,)), dma((4,)),
            dma((4,)), dma((4,)),
        ],
        compiler_params=pltpu.CompilerParams(
            collective_id=0, has_side_effects=True, vmem_limit_bytes=60 * 2**20
        ),
    )(hidden_in, down_weight, keep_mask)
    return layer_out, hessian


def solution(mesh):
    in_specs = (P("tok", "col"), P("col", "tok"), P("col", "tok"))
    out_specs = (P(("tok", "col"), None), P("col", "tok"))
    return jax.shard_map(body, mesh=mesh, in_specs=in_specs, out_specs=out_specs, check_vma=False)
```
